16 devices in a mesh: tp: 2 (over z), fsdp: 8 (over y, x, core).
Axes of the slice: x: 2, y: 2, z: 2, core: 2. Of those that a mesh axis runs over, the one named last changes fastest.
Arguments:
- emb_table: float32 [2048, 1152], P('tp', 'fsdp')
- tok_ids: int32 [32, 4096], P('fsdp')
- lab_ids: int32 [32, 4096], P('fsdp')
- h_last: bfloat16 [32, 4096, 1152], P('fsdp')
- g_embed: bfloat16 [32, 4096, 1152], P('fsdp')
- norm_w: float32 [1152], P('fsdp')
Outputs:
- output 1: bfloat16 [32, 4096, 1152], P('fsdp')
- output 2: float32 [], replicated
- output 3: bfloat16 [32, 4096, 1152], P('fsdp')
- output 4: float32 [1152], P('fsdp')
- output 5: float32 [2048, 1152], P('tp', 'fsdp')
All inputs are finite; a program needn't handle non-finite values.
Results may differ from the reference program's by a relative error of at most 0.001.
Values are sent between devices in bfloat16 or wider.
A program may use at most 1 GiB of HBM per device.

```python
import math
import jax
import jax.numpy as jnp
from jax import lax

D = 1152
VOCAB = 2048
BATCH = 32
SEQ = 4096

SOFT_CAP = 30.0
NORM_EPS = 1e-6
TOKENS = BATCH * SEQ
LEVELS = VOCAB.bit_length()
GRAD_STD = 12.0 / (TOKENS * math.sqrt(D))


def setup_inputs(seed: int = 0) -> dict:
    key_list = jax.random.split(jax.random.key(seed), 7)
    emb_table = jax.random.normal(key_list[0], (VOCAB, D), jnp.float32) * D ** -0.5
    tok_level = jax.random.randint(key_list[1], (BATCH, SEQ), 0, LEVELS)
    tok_upper = jnp.minimum(jnp.left_shift(jnp.full((BATCH, SEQ), 2, jnp.int32), tok_level), VOCAB)
    tok_ids = jax.random.randint(key_list[2], (BATCH, SEQ), 0, tok_upper)
    tok_ids = tok_ids.at[0, 0].set(VOCAB - 1).at[0, 1].set(0)
    lab_ids = jax.random.randint(key_list[3], (BATCH, SEQ), 0, VOCAB)
    lab_ids = lab_ids.at[BATCH - 1, SEQ - 1].set(VOCAB - 1).at[BATCH - 1, SEQ - 2].set(0)
    h_last = jax.random.normal(key_list[4], (BATCH, SEQ, D), jnp.float32).astype(jnp.bfloat16)
    g_embed = (jax.random.normal(key_list[5], (BATCH, SEQ, D), jnp.float32) * GRAD_STD).astype(jnp.bfloat16)
    norm_w = 15.0 + 5.0 * jax.random.normal(key_list[6], (D,), jnp.float32)
    return {"emb_table": emb_table, "tok_ids": tok_ids, "lab_ids": lab_ids, "h_last": h_last, "g_embed": g_embed, "norm_w": norm_w}


def reference(emb_table, tok_ids, lab_ids, h_last, g_embed, norm_w):
    table_bf = emb_table.astype(jnp.bfloat16)
    emb_scale = jnp.asarray(math.sqrt(D), jnp.bfloat16).astype(jnp.float32)
    x_emb = (jnp.take(table_bf, tok_ids, axis=0).astype(jnp.float32) * emb_scale).astype(jnp.bfloat16)
    norm_gain = 1.0 + norm_w
    vocab_ids = jnp.arange(VOCAB, dtype=jnp.int32)

    def row_step(d_acc, row_in):
        h_row, lab_row = row_in
        h_wide = h_row.astype(jnp.float32)
        inv_rms = lax.rsqrt(jnp.mean(h_wide * h_wide, axis=1, keepdims=True) + NORM_EPS)
        h_norm = h_wide * inv_rms
        x_norm = (h_norm * norm_gain).astype(jnp.bfloat16)
        logits = jnp.dot(x_norm, table_bf.T, preferred_element_type=jnp.float32)
        tanh_z = jnp.tanh(logits / SOFT_CAP)
        capped = SOFT_CAP * tanh_z
        log_norm = jax.nn.logsumexp(capped, axis=1)
        lab_hit = lab_row[:, None] == vocab_ids[None, :]
        lab_logit = jnp.sum(jnp.where(lab_hit, capped, 0.0), axis=1)
        soft_prob = jnp.exp(capped - log_norm[:, None])
        d_logits = ((soft_prob - lab_hit.astype(jnp.float32)) * (1.0 - tanh_z * tanh_z) / TOKENS).astype(jnp.bfloat16)
        d_xnorm = jnp.dot(d_logits, table_bf, preferred_element_type=jnp.float32)
        g_dir = d_xnorm * norm_gain
        d_hid = (inv_rms * (g_dir - h_norm * jnp.mean(g_dir * h_norm, axis=1, keepdims=True))).astype(jnp.bfloat16)
        d_gain = jnp.sum(d_xnorm * h_norm, axis=0)
        d_acc = d_acc + jnp.dot(d_logits.T, x_norm, preferred_element_type=jnp.float32)
        return d_acc, (jnp.sum(log_norm - lab_logit), d_hid, d_gain)

    d_head, (loss_rows, d_hidden, gain_rows) = lax.scan(row_step, jnp.zeros((VOCAB, D), jnp.float32), (h_last, lab_ids))
    loss_val = jnp.sum(loss_rows) / TOKENS
    d_norm_w = jnp.sum(gain_rows, axis=0)
    scaled_grad = (g_embed.astype(jnp.float32) * emb_scale).reshape(TOKENS, D)
    d_look = jax.ops.segment_sum(scaled_grad, tok_ids.reshape(TOKENS), num_segments=VOCAB)
    d_table = d_head + d_look
    return (x_emb, loss_val, d_hidden, d_norm_w, d_table)
```

```python
import functools
import math
import jax
import numpy as np
import jax.numpy as jnp
from jax import lax
from jax.experimental import pallas as pl
from jax.experimental.pallas import tpu as pltpu
from jax.sharding import PartitionSpec as P

SOFT_CAP = 30.0
NORM_EPS = 1e-6
LOG2E = 1.4426950408889634
TILE = 1024
GROUPS = 1
LOOK_TILE = 2048
GATHER_TILE = 2048
GATHER_GROUP = 128
LANES = 128
CHUNK = 1024
TN_DIMS = (((0,), (0,)), ((), ()))


def spread_ids(ids_ref):
    return jnp.transpose(jnp.broadcast_to(ids_ref[0], (LANES, ids_ref.shape[2])))


def lookup_grad_kernel(scale, row_ref, tok_ref, gx_ref, acc_ref, hit_ref):
    tile = gx_ref.shape[0]
    vocab_rows = acc_ref.shape[1]

    @pl.when(pl.program_id(0) == 0)
    def _():
        acc_ref[...] = jnp.zeros_like(acc_ref)

    tok_off = spread_ids(tok_ref) - row_ref[0] - lax.broadcasted_iota(jnp.int32, (tile, LANES), 1)
    for c in range(0, vocab_rows, LANES):
        hit_ref[:, c:c + LANES] = jnp.where(tok_off == c, scale, 0.0).astype(jnp.bfloat16)
    acc_ref[...] += lax.dot_general(gx_ref[...], hit_ref[...], TN_DIMS, preferred_element_type=jnp.float32)


def head_kernel(total_tokens, tp_ref, h_ref, lab_ref, gain_ref, table_t_ref, table_ref, init_ref,
                dh_ref, acc_ref, dg_ref, loss_ref, *sub_refs):
    tile, width = h_ref.shape
    halves, _, half_rows = table_t_ref.shape
    group = tile // GROUPS
    e_refs, dz_refs, xn_refs = (sub_refs[i * GROUPS:(i + 1) * GROUPS] for i in range(3))
    inv_n = 1.0 / total_tokens

    @pl.when(pl.program_id(0) == 0)
    def _():
        pltpu.sync_copy(init_ref, acc_ref.at[:, :half_rows])
        dg_ref[...] = jnp.zeros_like(dg_ref)
        loss_ref[...] = jnp.zeros_like(loss_ref)

    gain = gain_ref[...]
    lab_off = spread_ids(lab_ref) - lax.broadcasted_iota(jnp.int32, (tile, LANES), 1)
    rows = [slice(g * group, (g + 1) * group) for g in range(GROUPS)]
    inv_rms, sums, labs, lab_w, inv_sum, d_xnorm = ([None] * GROUPS for _ in range(6))

    def norm(g):
        h_wide = h_ref[rows[g], :].astype(jnp.float32)
        inv_rms[g] = lax.rsqrt(jnp.mean(h_wide * h_wide, axis=1, keepdims=True) + NORM_EPS)
        xn_refs[g][...] = (h_wide * inv_rms[g] * gain).astype(jnp.bfloat16)
        sums[g] = jnp.zeros((group, LANES), jnp.float32)
        labs[g] = jnp.zeros((group, LANES), jnp.float32)

    def logits(g, half, c):
        z = jnp.dot(xn_refs[g][...], table_t_ref[half, :, c:c + CHUNK], preferred_element_type=jnp.float32)
        for k in range(c, c + CHUNK, LANES):
            u = jnp.tanh(z[:, k - c:k - c + LANES] * (1.0 / SOFT_CAP))
            e = jnp.exp2((SOFT_CAP * LOG2E) * u)
            e_refs[g][half, :, k:k + LANES] = e * (1.0 - u * u)
            sums[g] += e
            labs[g] = jnp.where(lab_off[rows[g]] == half * half_rows + k, u, labs[g])

    def row_sums(g):
        sum_exp = jnp.sum(sums[g], axis=1, keepdims=True)
        lab_u = jnp.sum(labs[g], axis=1, keepdims=True)
        loss_ref[...] += jnp.log(sum_exp) - SOFT_CAP * lab_u
        inv_sum[g] = jnp.broadcast_to(inv_n / sum_exp, (group, LANES))
        lab_w[g] = jnp.broadcast_to((1.0 - lab_u * lab_u) * inv_n, (group, LANES))

    def d_logits(g, half, c):
        for k in range(c, c + CHUNK, LANES):
            hit = jnp.where(lab_off[rows[g]] == half * half_rows + k, lab_w[g], 0.0)
            dz_refs[g][half, :, k:k + LANES] = (e_refs[g][half, :, k:k + LANES] * inv_sum[g] - hit).astype(jnp.bfloat16)

    def d_xn(g, half):
        part = jnp.dot(dz_refs[g][half], table_ref[half], preferred_element_type=jnp.float32)
        d_xnorm[g] = part if half == 0 else d_xnorm[g] + part

    def d_tab(g):
        own = jnp.where(tp_ref[0] == 0, dz_refs[g][0], dz_refs[g][1])
        acc_ref[:, :half_rows] += lax.dot_general(xn_refs[g][...], own, TN_DIMS, preferred_element_type=jnp.float32)

    def d_hid(g):
        h_norm = h_ref[rows[g], :].astype(jnp.float32) * inv_rms[g]
        g_dir = d_xnorm[g] * gain
        mean_gh = jnp.mean(g_dir * h_norm, axis=1, keepdims=True)
        dh_ref[rows[g], :] = (inv_rms[g] * (g_dir - h_norm * mean_gh)).astype(jnp.bfloat16)
        dg_ref[...] += jnp.sum((d_xnorm[g] * h_norm).reshape(group // 8, 8, width), axis=0)

    chunks = [(half, c) for half in range(halves) for c in range(0, half_rows, CHUNK)]
    norm(0)
    for half, c in chunks:
        logits(0, half, c)
    row_sums(0)
    for half in range(halves):
        for c in range(0, half_rows, CHUNK):
            d_logits(0, half, c)
        d_xn(0, half)
    d_tab(0)
    d_hid(0)

    @pl.when(pl.program_id(0) == pl.num_programs(0) - 1)
    def _():
        dg_cols = jnp.transpose(jnp.broadcast_to(jnp.sum(dg_ref[...], axis=0, keepdims=True), (LANES, width)))
        loss_sum = jnp.sum(loss_ref[...], axis=0, keepdims=True)
        first_lane = lax.broadcasted_iota(jnp.int32, (width, LANES), 1) == 0
        acc_ref[:, half_rows:] = jnp.where(first_lane, dg_cols, loss_sum)


def lookup_kernel(tok_ref, table_ref, out_ref, rows_ref):
    tile = out_ref.shape[0]

    def group_step(g, _):
        base = pl.multiple_of(g * GATHER_GROUP, GATHER_GROUP)
        for t in range(GATHER_GROUP):
            rows_ref[t:t + 1, :] = table_ref[pl.ds(tok_ref[0, 0, base + t], 1), :]
        out_ref[pl.ds(base, GATHER_GROUP), :] = rows_ref[...].astype(jnp.bfloat16)
        return 0

    lax.fori_loop(0, tile // GATHER_GROUP, group_step, 0)


def solution(mesh):
    fsdp_size = mesh.shape["fsdp"]
    tp_size = mesh.shape["tp"]

    def device_step(emb_shard, tok_ids, lab_ids, h_last, g_embed, norm_w):
        vocab_rows, _ = emb_shard.shape
        batch_loc, seq_len, width = h_last.shape
        tok_count = batch_loc * seq_len
        total_tokens = tok_count * fsdp_size
        tp_index = lax.axis_index("tp")
        emb_scale = float(np.asarray(math.sqrt(width), jnp.bfloat16))
        h_rows = h_last.reshape(tok_count, width)
        gx_rows = g_embed.reshape(tok_count, width)
        tok_flat = tok_ids.reshape(tok_count)
        tok_rows = tok_ids.reshape(tok_count // LOOK_TILE, 1, LOOK_TILE)
        lab_rows = lab_ids.reshape(tok_count // TILE, 1, TILE)
        mm_flops = 2 * tok_count * width * vocab_rows

        shard_t = emb_shard.astype(jnp.bfloat16).T
        table_t = lax.all_gather(shard_t, ("tp", "fsdp"), axis=0, tiled=True).reshape(tp_size, width, vocab_rows)
        table = jnp.swapaxes(table_t, 1, 2)
        gain = (1.0 + lax.all_gather(norm_w, "fsdp", axis=0, tiled=True)).reshape(1, width)

        look_t = pl.pallas_call(
            functools.partial(lookup_grad_kernel, emb_scale),
            grid=(tok_count // LOOK_TILE,),
            in_specs=[
                pl.BlockSpec(memory_space=pltpu.SMEM),
                pl.BlockSpec((1, 1, LOOK_TILE), lambda i: (i, 0, 0)),
                pl.BlockSpec((LOOK_TILE, width), lambda i: (i, 0)),
            ],
            out_specs=pl.BlockSpec((width, vocab_rows), lambda i: (0, 0)),
            out_shape=jax.ShapeDtypeStruct((width, vocab_rows), jnp.float32),
            scratch_shapes=[pltpu.VMEM((LOOK_TILE, vocab_rows), jnp.bfloat16)],
            compiler_params=pltpu.CompilerParams(dimension_semantics=("arbitrary",), vmem_limit_bytes=60 * 2**20),
            cost_estimate=pl.CostEstimate(flops=mm_flops, bytes_accessed=tok_count * width * 2, transcendentals=0),
            name="lookup_grad",
        )((tp_index * vocab_rows).reshape(1).astype(jnp.int32), tok_rows, gx_rows)

        once = pl.Buffered(1)
        d_hidden, sums_t = pl.pallas_call(
            functools.partial(head_kernel, total_tokens),
            grid=(tok_count // TILE,),
            in_specs=[
                pl.BlockSpec(memory_space=pltpu.SMEM),
                pl.BlockSpec((TILE, width), lambda i: (i, 0)),
                pl.BlockSpec((1, 1, TILE), lambda i: (i, 0, 0)),
                pl.BlockSpec((1, width), lambda i: (0, 0)),
                pl.BlockSpec((tp_size, width, vocab_rows), lambda i: (0, 0, 0), pipeline_mode=once),
                pl.BlockSpec((tp_size, vocab_rows, width), lambda i: (0, 0, 0), pipeline_mode=once),
                pl.BlockSpec(memory_space=pl.ANY),
            ],
            out_specs=[
                pl.BlockSpec((TILE, width), lambda i: (i, 0)),
                pl.BlockSpec((width, vocab_rows + LANES), lambda i: (0, 0), pipeline_mode=once),
            ],
            out_shape=[
                jax.ShapeDtypeStruct((tok_count, width), jnp.bfloat16),
                jax.ShapeDtypeStruct((width, vocab_rows + LANES), jnp.float32),
            ],
            scratch_shapes=[
                pltpu.VMEM((8, width), jnp.float32),
                pltpu.VMEM((TILE // GROUPS, 1), jnp.float32),
                *[pltpu.VMEM((tp_size, TILE // GROUPS, vocab_rows), jnp.float32)] * GROUPS,
                *[pltpu.VMEM((tp_size, TILE // GROUPS, vocab_rows), jnp.bfloat16)] * GROUPS,
                *[pltpu.VMEM((TILE // GROUPS, width), jnp.bfloat16)] * GROUPS,
            ],
            compiler_params=pltpu.CompilerParams(dimension_semantics=("arbitrary",), vmem_limit_bytes=63 * 2**20),
            cost_estimate=pl.CostEstimate(flops=5 * mm_flops, bytes_accessed=tok_count * width * 4, transcendentals=0),
            name="head",
        )(tp_index.reshape(1).astype(jnp.int32), h_rows, lab_rows, gain, table_t, table, look_t)

        sums = lax.psum_scatter(sums_t, "fsdp", scatter_dimension=0, tiled=True)
        d_table = sums[:, :vocab_rows].T
        d_norm_w = sums[:, vocab_rows]
        loss_val = sums[0, vocab_rows + 1] / total_tokens

        scaled = (table.reshape(tp_size * vocab_rows, width).astype(jnp.float32) * emb_scale).astype(jnp.bfloat16).astype(jnp.float32)
        tok_late, _ = lax.optimization_barrier((tok_flat, sums_t[0, 0]))
        x_emb = pl.pallas_call(
            lookup_kernel,
            grid=(tok_count // GATHER_TILE,),
            in_specs=[
                pl.BlockSpec((1, 1, GATHER_TILE), lambda i: (i, 0, 0), memory_space=pltpu.SMEM),
                pl.BlockSpec((tp_size * vocab_rows, width), lambda i: (0, 0), pipeline_mode=once),
            ],
            out_specs=pl.BlockSpec((GATHER_TILE, width), lambda i: (i, 0)),
            out_shape=jax.ShapeDtypeStruct((tok_count, width), jnp.bfloat16),
            scratch_shapes=[pltpu.VMEM((GATHER_GROUP, width), jnp.float32)],
            compiler_params=pltpu.CompilerParams(dimension_semantics=("arbitrary",), vmem_limit_bytes=48 * 2**20),
            cost_estimate=pl.CostEstimate(flops=2 * mm_flops, bytes_accessed=tok_count * width * 2, transcendentals=0),
            name="lookup",
        )(tok_late.reshape(tok_count // GATHER_TILE, 1, GATHER_TILE), scaled)
        return (x_emb.reshape(batch_loc, seq_len, width), loss_val, d_hidden.reshape(batch_loc, seq_len, width), d_norm_w, d_table)

    spec_tok = P("fsdp", None)
    spec_act = P("fsdp", None, None)
    return jax.shard_map(device_step, mesh=mesh, in_specs=(P("tp", "fsdp"), spec_tok, spec_tok, spec_act, spec_act, P("fsdp")), out_specs=(spec_act, P(), spec_act, P("fsdp"), P("tp", "fsdp")), check_vma=False)
```
